16 devices in a mesh: dp: 2 (over z), tp: 8 (over y, x, core).
Axes of the slice: x: 2, y: 2, z: 2, core: 2. Of those that a mesh axis runs over, the one named last changes fastest.
Arguments:
- x_in: bfloat16 [2048, 4096], P('dp'), parts along dimension 0
- h_mid: bfloat16 [2048, 4096], P('dp'), parts along dimension 0
- mean_x: float32 [2048], P('dp'), parts along dimension 0
- rstd_x: float32 [2048], P('dp'), parts along dimension 0
- mean_h: float32 [2048], P('dp'), parts along dimension 0
- rstd_h: float32 [2048], P('dp'), parts along dimension 0
- gain_x: bfloat16 [4096], replicated
- gain_h: bfloat16 [4096], replicated
- w_qkv: bfloat16 [4096, 6144], P(None, 'tp')
- w_out: bfloat16 [32, 128, 4096], P('tp')
- w_gate: bfloat16 [4096, 14336], P(None, 'tp')
- w_up: bfloat16 [4096, 14336], P(None, 'tp')
- w_down: bfloat16 [14336, 4096], P('tp')
- d_out: bfloat16 [2048, 4096], P('dp'), parts along dimension 0
Outputs:
- output 1: bfloat16 [2048, 4096], P('dp'), parts along dimension 0
- output 2: bfloat16 [8192, 6144], P('dp', 'tp'), parts along dimension 0
- output 3: bfloat16 [64, 128, 4096], P(('dp', 'tp')), parts along dimension 0
- output 4: bfloat16 [8192, 14336], P('dp', 'tp'), parts along dimension 0
- output 5: bfloat16 [8192, 14336], P('dp', 'tp'), parts along dimension 0
- output 6: bfloat16 [28672, 4096], P(('dp', 'tp')), parts along dimension 0
There are 2 independent parts. The reference program is written for one: setup_inputs(seed, part) draws one part's arguments, and reference() takes and returns one part's arrays. A program takes and returns all parts, laid end to end along the dimension named above; an argument that names none is the same for every part.
All inputs are finite; a program needn't handle non-finite values.
Results may differ from the reference program's by a relative error of at most 0.0159252.
Values are sent between devices in bfloat16 or wider.
A program may use at most 1 GiB of HBM per device.

```python
import jax
import jax.numpy as jnp
from jax import lax

D = 4096
HEADS = 32
KV_HEADS = 8
HEAD = 128
FF = 14336
TOKENS = 1024

GROUP_SIZE = HEADS // KV_HEADS
QKV_COLS = (HEADS + 2 * KV_HEADS) * HEAD


def norm_stats(src_rows):
    row_vals = src_rows.astype(jnp.float32)
    row_mean = jnp.mean(row_vals, axis=-1)
    row_var = jnp.mean(jnp.square(row_vals - row_mean[:, None]), axis=-1)
    return row_mean, lax.rsqrt(row_var + 1e-5)


def setup_inputs(seed: int = 0, part: int = 0) -> dict:
    part_keys = jax.random.split(jax.random.fold_in(jax.random.key(seed), part), 7)
    shared_keys = jax.random.split(jax.random.key(seed + 1), 7)
    x_shift = jax.random.normal(part_keys[0], (TOKENS, 1), jnp.float32)
    x_scale = jax.random.uniform(part_keys[1], (TOKENS, 1), jnp.float32, 0.5, 2.0)
    x_in = ((jax.random.normal(part_keys[2], (TOKENS, D), jnp.float32) + x_shift) * x_scale).astype(jnp.bfloat16)
    h_shift = jax.random.normal(part_keys[3], (TOKENS, 1), jnp.float32)
    h_scale = jax.random.uniform(part_keys[4], (TOKENS, 1), jnp.float32, 0.5, 2.0)
    h_mid = ((jax.random.normal(part_keys[5], (TOKENS, D), jnp.float32) + h_shift) * h_scale).astype(jnp.bfloat16)
    d_out = jax.random.normal(part_keys[6], (TOKENS, D), jnp.float32).astype(jnp.bfloat16)
    mean_x, rstd_x = norm_stats(x_in)
    mean_h, rstd_h = norm_stats(h_mid)
    gain_x = (0.6 + 0.8 * jax.random.uniform(shared_keys[0], (D,), jnp.float32)).astype(jnp.bfloat16)
    gain_h = (0.6 + 0.8 * jax.random.uniform(shared_keys[1], (D,), jnp.float32)).astype(jnp.bfloat16)
    w_qkv = (jax.random.normal(shared_keys[2], (D, QKV_COLS), jnp.float32) * D ** -0.5).astype(jnp.bfloat16)
    w_out = (jax.random.normal(shared_keys[3], (HEADS, HEAD, D), jnp.float32) * (HEADS * HEAD) ** -0.5).astype(jnp.bfloat16)
    w_gate = (jax.random.normal(shared_keys[4], (D, FF), jnp.float32) * D ** -0.5).astype(jnp.bfloat16)
    w_up = (jax.random.normal(shared_keys[5], (D, FF), jnp.float32) * D ** -0.5).astype(jnp.bfloat16)
    w_down = (jax.random.normal(shared_keys[6], (FF, D), jnp.float32) * FF ** -0.5).astype(jnp.bfloat16)
    return {'x_in': x_in, 'h_mid': h_mid, 'mean_x': mean_x, 'rstd_x': rstd_x, 'mean_h': mean_h, 'rstd_h': rstd_h, 'gain_x': gain_x, 'gain_h': gain_h, 'w_qkv': w_qkv, 'w_out': w_out, 'w_gate': w_gate, 'w_up': w_up, 'w_down': w_down, 'd_out': d_out}


def layer_norm(src_rows, row_mean, row_rstd, gain_vec):
    centred = (src_rows.astype(jnp.float32) - row_mean[:, None]) * row_rstd[:, None]
    return (centred * gain_vec.astype(jnp.float32)).astype(jnp.bfloat16)


def norm_backward(grad_n, src_rows, row_mean, row_rstd, gain_vec):
    centred = (src_rows.astype(jnp.float32) - row_mean[:, None]) * row_rstd[:, None]
    scaled = grad_n * gain_vec.astype(jnp.float32)
    mean_grad = jnp.mean(scaled, axis=-1, keepdims=True)
    mean_proj = jnp.mean(scaled * centred, axis=-1, keepdims=True)
    return row_rstd[:, None] * (scaled - mean_grad - centred * mean_proj)


def attend(queries, key_rows, value_rows):
    scores = jnp.einsum('tgd,sd->gts', queries, key_rows) * (HEAD ** -0.5)
    positions = jnp.arange(queries.shape[0])
    causal = positions[:, None] >= positions[None, :]
    attn_probs = jax.nn.softmax(jnp.where(causal, scores, -1e30), axis=-1)
    return jnp.einsum('gts,sd->tgd', attn_probs, value_rows)


def group_backward(operands):
    queries, key_rows, value_rows, grad_o = operands
    outputs, pullback = jax.vjp(attend, queries, key_rows, value_rows)
    grad_q, grad_k, grad_v = pullback(grad_o)
    return outputs, grad_q, grad_k, grad_v


def reference(x_in, h_mid, mean_x, rstd_x, mean_h, rstd_h, gain_x, gain_h, w_qkv, w_out, w_gate, w_up, w_down, d_out):
    norm_h = layer_norm(h_mid, mean_h, rstd_h, gain_h)
    gate_f = jnp.dot(norm_h, w_gate, preferred_element_type=jnp.float32).astype(jnp.bfloat16).astype(jnp.float32)
    up_f = jnp.dot(norm_h, w_up, preferred_element_type=jnp.float32).astype(jnp.bfloat16).astype(jnp.float32)
    sig_gate = jax.nn.sigmoid(gate_f)
    gate_act = gate_f * sig_gate
    hidden = (gate_act * up_f).astype(jnp.bfloat16)
    d_w_down = jnp.dot(hidden.T, d_out, preferred_element_type=jnp.float32).astype(jnp.bfloat16)
    d_hidden = jnp.dot(d_out, w_down.T, preferred_element_type=jnp.float32).astype(jnp.bfloat16).astype(jnp.float32)
    d_gate = (d_hidden * up_f * sig_gate * (1.0 + gate_f * (1.0 - sig_gate))).astype(jnp.bfloat16)
    d_up = (d_hidden * gate_act).astype(jnp.bfloat16)
    d_w_gate = jnp.dot(norm_h.T, d_gate, preferred_element_type=jnp.float32).astype(jnp.bfloat16)
    d_w_up = jnp.dot(norm_h.T, d_up, preferred_element_type=jnp.float32).astype(jnp.bfloat16)
    d_norm_h = jnp.dot(d_gate, w_gate.T, preferred_element_type=jnp.float32) + jnp.dot(d_up, w_up.T, preferred_element_type=jnp.float32)
    d_mid = d_out.astype(jnp.float32) + norm_backward(d_norm_h, h_mid, mean_h, rstd_h, gain_h)
    d_mid_b = d_mid.astype(jnp.bfloat16)
    norm_x = layer_norm(x_in, mean_x, rstd_x, gain_x)
    qkv_rows = jnp.dot(norm_x, w_qkv, preferred_element_type=jnp.float32).astype(jnp.bfloat16).astype(jnp.float32)
    qkv_rows = qkv_rows.reshape(TOKENS, KV_HEADS, GROUP_SIZE + 2, HEAD)
    queries = jnp.moveaxis(qkv_rows[:, :, :GROUP_SIZE], 1, 0)
    key_rows = jnp.moveaxis(qkv_rows[:, :, GROUP_SIZE], 1, 0)
    value_rows = jnp.moveaxis(qkv_rows[:, :, GROUP_SIZE + 1], 1, 0)
    d_heads = jnp.dot(d_mid_b, w_out.reshape(HEADS * HEAD, D).T, preferred_element_type=jnp.float32).astype(jnp.bfloat16).astype(jnp.float32)
    grad_o = jnp.moveaxis(d_heads.reshape(TOKENS, KV_HEADS, GROUP_SIZE, HEAD), 1, 0)
    outputs, grad_q, grad_k, grad_v = lax.map(group_backward, (queries, key_rows, value_rows, grad_o))
    attn_out = jnp.moveaxis(outputs, 0, 1).reshape(TOKENS, HEADS * HEAD).astype(jnp.bfloat16)
    d_w_out = jnp.dot(attn_out.T, d_mid_b, preferred_element_type=jnp.float32).astype(jnp.bfloat16).reshape(HEADS, HEAD, D)
    grad_qkv = jnp.concatenate([grad_q, grad_k[:, :, None], grad_v[:, :, None]], axis=2)
    d_qkv = jnp.moveaxis(grad_qkv, 0, 1).reshape(TOKENS, QKV_COLS).astype(jnp.bfloat16)
    d_w_qkv = jnp.dot(norm_x.T, d_qkv, preferred_element_type=jnp.float32).astype(jnp.bfloat16)
    d_norm_x = jnp.dot(d_qkv, w_qkv.T, preferred_element_type=jnp.float32)
    d_x = (d_mid + norm_backward(d_norm_x, x_in, mean_x, rstd_x, gain_x)).astype(jnp.bfloat16)
    return d_x, d_w_qkv, d_w_out, d_w_gate, d_w_up, d_w_down
```

```python
import functools

import jax
import jax.numpy as jnp
from jax import lax
from jax.experimental import pallas as pl
from jax.experimental.pallas import tpu as pltpu
from jax.sharding import PartitionSpec as P

F32 = jnp.float32
BF16 = jnp.bfloat16
VMEM_LIMIT = 62 * 1024 * 1024
ANY = pl.BlockSpec(memory_space=pl.ANY)
IN_VMEM = pl.BlockSpec(memory_space=pltpu.VMEM)


def dot(lhs, rhs, lhs_dim, rhs_dim):
    return lax.dot_general(lhs, rhs, (((lhs_dim,), (rhs_dim,)), ((), ())), preferred_element_type=F32)


def resident(shape):
    return pl.BlockSpec(shape, lambda i: (0,) * len(shape), pipeline_mode=pl.Buffered(1))


def shape_of(shape, dtype=BF16):
    return jax.ShapeDtypeStruct(shape, dtype)


def params(**kw):
    return pltpu.CompilerParams(vmem_limit_bytes=VMEM_LIMIT, **kw)


def normed(src, mean, rstd, gain):
    return (((src.astype(F32) - mean) * rstd) * gain.astype(F32)).astype(BF16)


def mlp_body(h_ref, st_ref, gain_ref, do_ref, wg_ref, wu_ref, wd_ref, hid_ref, dg_ref, du_ref, n_ref):
    rows = h_ref.shape[0]

    @pl.when(pl.program_id(0) == 0)
    def _():
        @pl.loop(0, rows // 128)
        def _(i):
            r = pl.ds(pl.multiple_of(i * 128, 128), 128)
            n_ref[r, :] = normed(h_ref[r, :], st_ref[r, 0:1], st_ref[r, 1:2], gain_ref[...])

    gate = dot(n_ref[...], wg_ref[...], 1, 0).astype(BF16).astype(F32)
    up = dot(n_ref[...], wu_ref[...], 1, 0).astype(BF16).astype(F32)
    d_hid = dot(do_ref[...], wd_ref[...], 1, 1).astype(BF16).astype(F32)
    sig = jax.nn.sigmoid(gate)
    act = gate * sig
    hid_ref[...] = (act * up).astype(BF16)
    dg_ref[...] = (d_hid * up * sig * (1.0 + gate * (1.0 - sig))).astype(BF16)
    du_ref[...] = (d_hid * act).astype(BF16)


def mlp_grads(h, stats, gain, d_out, wg, wu, wd, block=256):
    t, d = h.shape
    f = wg.shape[1]
    col = lambda n: pl.BlockSpec((n, block), lambda i: (0, i))
    return pl.pallas_call(
        mlp_body,
        grid=(f // block,),
        in_specs=[resident((t, d)), resident(stats.shape), resident(gain.shape), resident((t, d)),
                  col(d), col(d), pl.BlockSpec((block, d), lambda i: (i, 0))],
        out_specs=[col(t)] * 3 + [resident((t, d))],
        out_shape=[shape_of((t, f))] * 3 + [shape_of((t, d))],
        compiler_params=params(),
        name="mlp_grads",
    )(h, stats, gain, d_out, wg, wu, wd)


def part_body(dg_ref, du_ref, wg_ref, wu_ref, out_ref):
    out_ref[...] = (dot(dg_ref[...], wg_ref[...], 1, 1) + dot(du_ref[...], wu_ref[...], 1, 1)).astype(BF16)


def mlp_part(dg, du, wg, wu, block=512):
    t, f = dg.shape
    d = wg.shape[0]
    return pl.pallas_call(
        part_body,
        grid=(d // block,),
        in_specs=[resident((t, f)), resident((t, f))] + [pl.BlockSpec((block, f), lambda i: (i, 0))] * 2,
        out_specs=pl.BlockSpec((t, block), lambda i: (0, i)),
        out_shape=shape_of((t, d)),
        compiler_params=params(),
        name="mlp_part",
    )(dg, du, wg, wu)


def attention_body(qkv_ref, do_ref, o_ref, dqkv_ref, dk_acc, dv_acc, *, group, hd, chunk):
    total = qkv_ref.shape[0]
    chunks = total // chunk
    scale = hd ** -0.5

    @pl.when(pl.program_id(0) == 0)
    def _():
        dk_acc[...] = jnp.zeros_like(dk_acc)
        dv_acc[...] = jnp.zeros_like(dv_acc)

    for c in range(chunks):
        @pl.when(pl.program_id(0) == chunks - 1 - c)
        def _():
            kv = (c + 1) * chunk
            mine = slice(c * chunk, kv)
            keys = qkv_ref[0:kv, group * hd:(group + 1) * hd]
            vals = qkv_ref[0:kv, (group + 1) * hd:(group + 2) * hd]
            q_pos = c * chunk + lax.broadcasted_iota(jnp.int32, (chunk, kv), 0)
            causal = q_pos >= lax.broadcasted_iota(jnp.int32, (chunk, kv), 1)
            for h in range(group):
                cols = slice(h * hd, (h + 1) * hd)
                q = qkv_ref[mine, cols]
                do = do_ref[:, cols]
                s = jnp.where(causal, dot(q, keys, 1, 1) * scale, -1e30)
                e = jnp.exp(s - jnp.max(s, axis=1, keepdims=True))
                p = e * (1.0 / jnp.sum(e, axis=1, keepdims=True))
                p_low = p.astype(BF16)
                o_ref[:, cols] = dot(p_low, vals, 1, 0).astype(BF16)
                dp = dot(do, vals, 1, 1)
                row_dot = jnp.sum(p * dp, axis=1, keepdims=True)
                ds = (p * (dp - row_dot) * scale).astype(BF16)
                dqkv_ref[:, cols] = dot(ds, keys, 1, 0).astype(BF16)
                dk_acc[:, 0:kv] += dot(q, ds, 0, 0)
                dv_acc[:, 0:kv] += dot(do, p_low, 0, 0)
            dqkv_ref[:, group * hd:(group + 1) * hd] = dk_acc[:, mine].T.astype(BF16)
            dqkv_ref[:, (group + 1) * hd:(group + 2) * hd] = dv_acc[:, mine].T.astype(BF16)


def attention(qkv, d_heads, hd, chunk=256):
    t, c = qkv.shape
    group = c // hd - 2
    n = t // chunk
    back = lambda w: pl.BlockSpec((chunk, w), lambda i: (n - 1 - i, 0))
    return pl.pallas_call(
        functools.partial(attention_body, group=group, hd=hd, chunk=chunk),
        grid=(n,),
        in_specs=[resident((t, c)), back(group * hd)],
        out_specs=[back(group * hd), back(c)],
        out_shape=[shape_of((t, group * hd)), shape_of((t, c))],
        scratch_shapes=[pltpu.VMEM((hd, t), F32), pltpu.VMEM((hd, t), F32)],
        compiler_params=params(),
        name="attention",
    )(qkv, d_heads)


CORE, XN, YN, DIAG = 1, 2, 4, 6
ORDER = (DIAG, XN, YN, 0)


def exchange_scratch(rows, d, base_dtype):
    half = rows // 2
    return [
        pltpu.VMEM((4, rows, d), BF16),
        pltpu.VMEM((4, rows, d), BF16),
        pltpu.VMEM((2, half, d), BF16),
        pltpu.VMEM((2, rows, d), BF16),
        pltpu.VMEM((rows, d), BF16),
        pltpu.VMEM((rows, d), BF16),
        pltpu.VMEM((rows, d), base_dtype),
        pltpu.VMEM((rows, d), F32),
        pltpu.SemaphoreType.DMA((8,)),
        pltpu.SemaphoreType.DMA((32,)),
        pltpu.SemaphoreType.DMA((32,)),
    ]


class Exchange:
    def __init__(self, rows, part, z, base, base_row, st, st_col, gain, full, own, scratch):
        self.rows, self.half = rows, rows // 2
        self.part, self.z, self.base, self.base_row = part, z, base, base_row
        self.st, self.st_col, self.gain, self.full, self.own = st, st_col, gain, full, own
        (self.from_core, self.sums, self.via, self.mine, self.res, self.zv, self.bv, self.resf,
         self.lsem, self.ssem, self.rsem) = scratch
        self.me = lax.axis_index("tp")

    def peer(self, rel):
        return lax.bitwise_xor(self.me, rel)

    def block(self, rel, lo=0, n=None):
        n = self.rows if n is None else n
        return pl.ds(pl.multiple_of(self.peer(rel) * self.rows + lo, 16), n)

    def remote(self, k, src, dst, rel):
        return pltpu.make_async_remote_copy(
            src_ref=src, dst_ref=dst, send_sem=self.ssem.at[k], recv_sem=self.rsem.at[k],
            device_id={"tp": self.peer(rel)}, device_id_type=pl.DeviceIdType.MESH)

    def core_copy(self, j):
        return self.remote(j, self.part.at[self.block(ORDER[j] ^ CORE)], self.from_core.at[j], CORE)

    def local_copy(self, j):
        return pltpu.make_async_copy(self.part.at[self.block(ORDER[j])], self.sums.at[j], self.lsem.at[j])

    def side_copies(self):
        r = self.rows
        at = self.me * r if self.base_row is None else self.base_row
        return (pltpu.make_async_copy(self.z.at[self.block(0)], self.zv, self.lsem.at[4]),
                pltpu.make_async_copy(self.base.at[pl.ds(at, r)], self.bv, self.lsem.at[5]))

    def scatter_copy(self, k):
        lo, hi = pl.ds(0, self.half), pl.ds(self.half, self.half)
        src, dst, rel = {
            4: (self.sums.at[0, lo], self.via.at[0], XN),
            5: (self.sums.at[0, hi], self.via.at[1], YN),
            6: (self.sums.at[1, lo], self.mine.at[0, lo], XN),
            7: (self.sums.at[2, hi], self.mine.at[1, hi], YN),
            8: (self.sums.at[1, hi], self.mine.at[0, hi], XN),
            9: (self.sums.at[2, lo], self.mine.at[1, lo], YN),
        }[k]
        return self.remote(k, src, dst, rel)

    def gather_copy(self, k):
        n = self.half
        src_rel, lo, cnt, to, from_res = {
            10: (0, 0, n, XN, True), 11: (0, n, n, XN, True),
            12: (0, n, n, YN, True), 13: (0, 0, n, YN, True),
            14: (0, 0, 2 * n, CORE, True),
            15: (YN, n, n, XN, False), 16: (XN, 0, n, YN, False),
            17: (XN, 0, n, CORE, False), 18: (XN, n, n, CORE, False),
            19: (YN, n, n, CORE, False), 20: (YN, 0, n, CORE, False),
            21: (DIAG, n, n, CORE, False), 22: (DIAG, 0, n, CORE, False),
        }[k]
        dst = self.full.at[self.block(src_rel, lo, cnt)]
        return self.remote(k, self.res.at[pl.ds(lo, cnt)] if from_res else dst, dst, to)

    def start(self):
        barrier = pltpu.get_barrier_semaphore()
        for rel in (CORE, XN, YN):
            pl.semaphore_signal(barrier, inc=1, device_id={"tp": self.peer(rel)}, device_id_type=pl.DeviceIdType.MESH)
        pl.semaphore_wait(barrier, 3)
        for j in range(4):
            self.core_copy(j).start()
            self.local_copy(j).start()
        for c in self.side_copies():
            c.start()

    def add(self, dst, src):
        n = dst.shape[0]

        @pl.loop(0, n // 16)
        def _(i):
            r = pl.ds(pl.multiple_of(i * 16, 16), 16)
            dst[r, :] = (dst[r, :].astype(F32) + src[r, :].astype(F32)).astype(BF16)

    def chip_sums(self):
        for j in range(4):
            self.local_copy(j).wait()
            self.core_copy(j).wait_recv()
            self.add(self.sums.at[j], self.from_core.at[j])
            for k in {0: (4, 5), 1: (6,), 2: (7,), 3: ()}[j]:
                self.scatter_copy(k).start()

    def forward_sums(self):
        lo, hi = pl.ds(0, self.half), pl.ds(self.half, self.half)
        self.scatter_copy(5).wait_recv()
        self.add(self.sums.at[1, hi], self.via.at[1])
        self.scatter_copy(8).start()
        self.scatter_copy(4).wait_recv()
        self.add(self.sums.at[2, lo], self.via.at[0])
        self.scatter_copy(9).start()

    def norm_and_send(self):
        for k in (6, 7, 8, 9):
            self.scatter_copy(k).wait_recv()
        for c in self.side_copies():
            c.wait()
        gain = self.gain[...].astype(F32)
        base = self.me * self.rows

        @pl.loop(0, self.rows // 16)
        def _(i):
            r = pl.ds(pl.multiple_of(i * 16, 16), 16)
            g = pl.ds(pl.multiple_of(base + i * 16, 16), 16)
            mean = self.st[g, self.st_col:self.st_col + 1]
            rstd = self.st[g, self.st_col + 1:self.st_col + 2]
            grad = self.sums[3, r, :].astype(F32) + self.mine[0, r, :].astype(F32) + self.mine[1, r, :].astype(F32)
            zh = (self.zv[r, :].astype(F32) - mean) * rstd
            u = grad * gain
            mean_u = jnp.mean(u, axis=1, keepdims=True)
            mean_p = jnp.mean(u * zh, axis=1, keepdims=True)
            out = self.bv[r, :].astype(F32) + rstd * (u - mean_u - zh * mean_p)
            self.resf[r, :] = out
            self.res[r, :] = out.astype(BF16)
        for k in (10, 12, 11, 13, 14):
            self.gather_copy(k).start()
        self.keep()[0].start()
        if self.own is not None:
            self.keep()[1].start()

    def keep(self):
        c = [pltpu.make_async_copy(self.res, self.full.at[self.block(0)], self.lsem.at[6])]
        if self.own is not None:
            c.append(pltpu.make_async_copy(self.resf, self.own, self.lsem.at[7]))
        return c

    def forward_first(self):
        self.gather_copy(10).wait_recv()
        self.gather_copy(16).start()
        self.gather_copy(12).wait_recv()
        self.gather_copy(15).start()
        self.gather_copy(17).start()
        self.gather_copy(19).start()

    def forward_second(self):
        self.gather_copy(11).wait_recv()
        self.gather_copy(18).start()
        self.gather_copy(13).wait_recv()
        self.gather_copy(20).start()

    def finish(self):
        self.gather_copy(15).wait_recv()
        self.gather_copy(21).start()
        self.gather_copy(16).wait_recv()
        self.gather_copy(22).start()
        for k in (14, 17, 18, 19, 20, 21, 22):
            self.gather_copy(k).wait_recv()
        for j in range(4):
            self.core_copy(j).wait_send()
        for k in range(4, 10):
            self.scatter_copy(k).wait_send()
        for k in range(10, 23):
            self.gather_copy(k).wait_send()
        for c in self.keep():
            c.wait()

    def events(self):
        return [self.chip_sums, self.forward_sums, self.norm_and_send, self.forward_first, self.forward_second,
                self.finish]


def run_phases(ex, phases, when):
    events = list(zip(when, ex.events()))
    ex.start()
    done = 0
    for body, steps, in_specs, out_specs, refs in phases:
        here = [(w - done, e) for w, e in events if done <= w < done + steps]

        def step(*tiles, body=body, here=here):
            for w, e in here:
                pl.when(pl.program_id(0) == w)(e)
            body(*tiles)

        pltpu.emit_pipeline(step, grid=(steps,), in_specs=in_specs, out_specs=out_specs)(*refs)
        done += steps
    for w, e in events:
        if w >= done:
            e()


def rows_spec(n, w):
    return pl.BlockSpec((n, w), lambda i: (i, 0))


def cols_spec(h, n):
    return pl.BlockSpec((h, n), lambda i: (0, i))


def first_body(part, z, base, st, gain_h, gain_x, n, dg, du, x, wqkv,
               full, own, dwg, dwu, nx, qkv, dgv, duv, wv, wsem, *scratch, rows, when):
    t, d = z.shape
    f = dg.shape[1]
    c = wqkv.shape[1]
    ex = Exchange(rows, part, z, base, None, st, 0, gain_h, full, own, scratch)
    loads = [pltpu.make_async_copy(s, v, wsem.at[i]) for i, (s, v) in enumerate(((dg, dgv), (du, duv), (wqkv, wv)))]
    for l in loads:
        l.start()
    for l in loads:
        l.wait()

    def weight_grads(n_t, g_t, u_t):
        g_t[...] = dot(n_t[...], dgv[...], 0, 0).astype(BF16)
        u_t[...] = dot(n_t[...], duv[...], 0, 0).astype(BF16)

    def project(x_t, s_t, n_t, q_t):
        n_t[...] = normed(x_t[...], s_t[:, 2:3], s_t[:, 3:4], gain_x[...])
        q_t[...] = dot(n_t[...], wv[...], 1, 0).astype(BF16)

    rb = 256
    phases = [
        (weight_grads, d // 256, [cols_spec(t, 256)], [rows_spec(256, f)] * 2, (n, dwg, dwu)),
        (project, t // rb, [rows_spec(rb, d), rows_spec(rb, 4)], [rows_spec(rb, d), rows_spec(rb, c)], (x, st, nx, qkv)),
    ]
    run_phases(ex, phases, when)


def first_exchange(part, h, d_out, stats, gain_h, gain_x, n, dg, du, x, wqkv, tp):
    t, d = h.shape
    f = dg.shape[1]
    c = wqkv.shape[1]
    rows = t // tp
    return pl.pallas_call(
        functools.partial(first_body, rows=rows, when=(4, 10, 19, 26, 30, 34)),
        in_specs=[ANY, ANY, ANY, IN_VMEM, IN_VMEM, IN_VMEM, ANY, ANY, ANY, ANY, ANY],
        out_specs=[ANY] * 6,
        out_shape=[shape_of((t, d)), shape_of((rows, d), F32), shape_of((d, f)), shape_of((d, f)),
                   shape_of((t, d)), shape_of((t, c))],
        scratch_shapes=[pltpu.VMEM((t, f), BF16), pltpu.VMEM((t, f), BF16), pltpu.VMEM((d, c), BF16),
                        pltpu.SemaphoreType.DMA((3,))] + exchange_scratch(rows, d, BF16),
        compiler_params=params(collective_id=1, has_side_effects=True),
        name="first_exchange",
    )(part, h, d_out, stats, gain_h, gain_x, n, dg, du, x, wqkv)


def second_body(part, z, base, st, gain_x, hid, d_out, nx, dqkv, o, dmid,
                full, dwd, dwqkv, dwo, hidv, dqv, ov, wsem, *scratch, rows, when):
    t, d = z.shape
    f = hid.shape[1]
    c = dqkv.shape[1]
    hw = o.shape[1]
    ex = Exchange(rows, part, z, base, 0, st, 2, gain_x, full, None, scratch)
    loads = [pltpu.make_async_copy(s, v, wsem.at[i]) for i, (s, v) in enumerate(((hid, hidv), (dqkv, dqv), (o, ov)))]
    for l in loads:
        l.start()
    for l in loads:
        l.wait()

    def down(do_t, out_t):
        out_t[...] = dot(hidv[...], do_t[...], 0, 0).astype(BF16)

    def qkv_grad(n_t, out_t):
        out_t[...] = dot(n_t[...], dqv[...], 0, 0).astype(BF16)

    def out_grad(dm_t, out_t):
        out_t[...] = dot(ov[...], dm_t[...], 0, 0).astype(BF16)

    phases = [
        (down, d // 512, [cols_spec(t, 512)], [cols_spec(f, 512)], (d_out, dwd)),
        (qkv_grad, d // 512, [cols_spec(t, 512)], [rows_spec(512, c)], (nx, dwqkv)),
        (out_grad, d // 512, [cols_spec(t, 512)], [cols_spec(hw, 512)], (dmid, dwo)),
    ]
    run_phases(ex, phases, when)


def second_exchange(part, x, own, stats, gain_x, hid, d_out, nx, dqkv, o, dmid, tp):
    t, d = x.shape
    f = hid.shape[1]
    c = dqkv.shape[1]
    hw = o.shape[1]
    rows = t // tp
    return pl.pallas_call(
        functools.partial(second_body, rows=rows, when=(3, 9, 24, 25, 26, 27)),
        in_specs=[ANY, ANY, ANY, IN_VMEM, IN_VMEM, ANY, ANY, ANY, ANY, ANY, ANY],
        out_specs=[ANY] * 4,
        out_shape=[shape_of((t, d)), shape_of((f, d)), shape_of((d, c)), shape_of((hw, d))],
        scratch_shapes=[pltpu.VMEM((t, f), BF16), pltpu.VMEM((t, c), BF16), pltpu.VMEM((t, hw), BF16),
                        pltpu.SemaphoreType.DMA((3,))] + exchange_scratch(rows, d, F32),
        compiler_params=params(collective_id=2, has_side_effects=True),
        name="second_exchange",
    )(part, x, own, stats, gain_x, hid, d_out, nx, dqkv, o, dmid)


def solution(mesh):
    tp = mesh.shape["tp"]

    def device_step(x_in, h_mid, mean_x, rstd_x, mean_h, rstd_h, gain_x, gain_h, w_qkv, w_out, w_gate, w_up, w_down, d_out):
        heads, hd, d = w_out.shape
        stats = jnp.stack([mean_h, rstd_h, mean_x, rstd_x], axis=1)
        gx, gh = gain_x.reshape(1, d), gain_h.reshape(1, d)
        w_o = w_out.reshape(heads * hd, d)
        hid, d_gate, d_up, norm_h = mlp_grads(h_mid, stats, gh, d_out, w_gate, w_up, w_down)
        part_h = mlp_part(d_gate, d_up, w_gate, w_up)
        d_mid_b, own, d_w_gate, d_w_up, norm_x, qkv = first_exchange(
            part_h, h_mid, d_out, stats, gh, gx, norm_h, d_gate, d_up, x_in, w_qkv, tp)
        d_heads = jnp.einsum('te,he->th', d_mid_b, w_o, preferred_element_type=F32).astype(BF16)
        o, d_qkv = attention(qkv, d_heads, hd)
        part_x = jnp.einsum('tc,dc->td', d_qkv, w_qkv, preferred_element_type=F32).astype(BF16)
        d_x, d_w_down, d_w_qkv, d_w_out = second_exchange(
            part_x, x_in, own, stats, gx, hid, d_out, norm_x, d_qkv, o, d_mid_b, tp)
        return d_x, d_w_qkv, d_w_out.reshape(w_out.shape), d_w_gate, d_w_up, d_w_down

    row_spec = P('dp', None)
    stat_spec = P('dp')
    col_spec = P(None, 'tp')
    in_specs = (row_spec, row_spec, stat_spec, stat_spec, stat_spec, stat_spec, P(None), P(None), col_spec, P('tp', None, None), col_spec, col_spec, P('tp', None), row_spec)
    out_specs = (row_spec, P('dp', 'tp'), P(('dp', 'tp'), None, None), P('dp', 'tp'), P('dp', 'tp'), P(('dp', 'tp'), None))
    return jax.shard_map(device_step, mesh=mesh, in_specs=in_specs, out_specs=out_specs, check_vma=False)
```

```python
import functools

import jax
import jax.numpy as jnp
from jax import lax
from jax.experimental import pallas as pl
from jax.experimental.pallas import tpu as pltpu
from jax.sharding import PartitionSpec as P

F32 = jnp.float32
BF16 = jnp.bfloat16
VMEM_LIMIT = 62 * 1024 * 1024
ANY = pl.BlockSpec(memory_space=pl.ANY)
IN_VMEM = pl.BlockSpec(memory_space=pltpu.VMEM)


def dot(lhs, rhs, lhs_dim, rhs_dim):
    return lax.dot_general(lhs, rhs, (((lhs_dim,), (rhs_dim,)), ((), ())), preferred_element_type=F32)


def resident(shape):
    return pl.BlockSpec(shape, lambda i: (0,) * len(shape), pipeline_mode=pl.Buffered(1))


def shape_of(shape, dtype=BF16):
    return jax.ShapeDtypeStruct(shape, dtype)


def params(**kw):
    return pltpu.CompilerParams(vmem_limit_bytes=VMEM_LIMIT, **kw)


def normed(src, mean, rstd, gain):
    return (((src.astype(F32) - mean) * rstd) * gain.astype(F32)).astype(BF16)


def swiglu_grads(n, d_out, wg, wu, wd):
    gate = dot(n, wg, 1, 0).astype(BF16).astype(F32)
    up = dot(n, wu, 1, 0).astype(BF16).astype(F32)
    d_hid = dot(d_out, wd, 1, 1).astype(BF16).astype(F32)
    sig = jax.nn.sigmoid(gate)
    act = gate * sig
    return ((act * up).astype(BF16), (d_hid * up * sig * (1.0 + gate * (1.0 - sig))).astype(BF16),
            (d_hid * act).astype(BF16))


def mlp_body(h_ref, st_ref, gain_ref, do_ref, wg_ref, wu_ref, wd_ref, hid_ref, dg_ref, du_ref, n_ref):
    rows = h_ref.shape[0]
    upper = slice(rows // 2, rows)

    @pl.when(pl.program_id(0) == 0)
    def _():
        @pl.loop(0, rows // 128)
        def _(i):
            r = pl.ds(pl.multiple_of(i * 128, 128), 128)
            n_ref[r, :] = normed(h_ref[r, :], st_ref[r, 0:1], st_ref[r, 1:2], gain_ref[...])

    hid_ref[...], dg_ref[...], du_ref[...] = swiglu_grads(n_ref[upper, :], do_ref[...], wg_ref[...], wu_ref[...], wd_ref[...])


def mlp_grads(h, stats, gain, d_out, wg, wu, wd, block=256):
    t, d = h.shape
    f = wg.shape[1]
    col = lambda n: pl.BlockSpec((n, block), lambda i: (0, i))
    return pl.pallas_call(
        mlp_body,
        grid=(f // block,),
        in_specs=[resident((t, d)), resident(stats.shape), resident(gain.shape), pl.BlockSpec((t // 2, d), lambda i: (1, 0), pipeline_mode=pl.Buffered(1)),
                  col(d), col(d), pl.BlockSpec((block, d), lambda i: (i, 0))],
        out_specs=[col(t // 2)] * 3 + [resident((t, d))],
        out_shape=[shape_of((t // 2, f))] * 3 + [shape_of((t, d))],
        compiler_params=params(),
        name="mlp_grads",
    )(h, stats, gain, d_out, wg, wu, wd)


def part_body(dg_ref, du_ref, wg_ref, wu_ref, out_ref):
    out_ref[...] = (dot(dg_ref[...], wg_ref[...], 1, 1) + dot(du_ref[...], wu_ref[...], 1, 1)).astype(BF16)


def mlp_part(dg, du, wg, wu, block=512):
    t, f = dg.shape
    d = wg.shape[0]
    return pl.pallas_call(
        part_body,
        grid=(d // block,),
        in_specs=[resident((t, f)), resident((t, f))] + [pl.BlockSpec((block, f), lambda i: (i, 0))] * 2,
        out_specs=pl.BlockSpec((t, block), lambda i: (0, i)),
        out_shape=shape_of((t, d)),
        compiler_params=params(),
        name="mlp_part",
    )(dg, du, wg, wu)


CORE, XN, YN, DIAG = 1, 2, 4, 6
ORDER = (DIAG, XN, YN, 0)
COPIES = 24


def exchange_scratch(rows, d):
    half = rows // 2
    return [
        pltpu.VMEM((4, rows, d), BF16),
        pltpu.VMEM((4, rows, d), BF16),
        pltpu.VMEM((2, half, d), BF16),
        pltpu.VMEM((2, rows, d), BF16),
        pltpu.VMEM((rows, d), BF16),
        pltpu.VMEM((rows, d), BF16),
        pltpu.VMEM((rows, d), BF16),
        pltpu.VMEM((rows, d), F32),
    ]


class Exchange:
    def __init__(self, index, rows, row0, part, part0, z, base, st, st_col, gain, full, scratch, sems):
        self.index, self.rows, self.half, self.row0 = index, rows, rows // 2, row0
        self.part, self.part0, self.z, self.base = part, part0, z, base
        self.st, self.st_col, self.gain, self.full = st, st_col, gain, full
        self.from_core, self.sums, self.via, self.mine, self.res, self.zv, self.bv, self.resf = scratch
        self.lsem, self.ssem, self.rsem = sems
        self.me = lax.axis_index("tp")

    def peer(self, rel):
        return lax.bitwise_xor(self.me, rel)

    def block(self, rel, base, lo=0, n=None):
        n = self.rows if n is None else n
        return pl.ds(pl.multiple_of(self.peer(rel) * self.rows + base + lo, 16), n)

    def remote(self, k, src, dst, rel):
        k = self.index * COPIES + k
        return pltpu.make_async_remote_copy(
            src_ref=src, dst_ref=dst, send_sem=self.ssem.at[k], recv_sem=self.rsem.at[k],
            device_id={"tp": self.peer(rel)}, device_id_type=pl.DeviceIdType.MESH)

    def local(self, k, src, dst):
        return pltpu.make_async_copy(src, dst, self.lsem.at[self.index * 8 + k])

    def core_copy(self, j):
        return self.remote(j, self.part.at[self.block(ORDER[j] ^ CORE, self.part0)], self.from_core.at[j], CORE)

    def local_copy(self, j):
        return self.local(j, self.part.at[self.block(ORDER[j], self.part0)], self.sums.at[j])

    def side_copy(self, k):
        if k == 0:
            return self.local(4, self.z.at[self.block(0, self.row0)], self.zv)
        return self.local(5, self.base.at[self.block(0, self.row0)], self.bv)

    def scatter_copy(self, k):
        lo, hi = pl.ds(0, self.half), pl.ds(self.half, self.half)
        src, dst, rel = {
            4: (self.sums.at[0, lo], self.via.at[0], XN),
            5: (self.sums.at[0, hi], self.via.at[1], YN),
            6: (self.sums.at[1, lo], self.mine.at[0, lo], XN),
            7: (self.sums.at[2, hi], self.mine.at[1, hi], YN),
            8: (self.sums.at[1, hi], self.mine.at[0, hi], XN),
            9: (self.sums.at[2, lo], self.mine.at[1, lo], YN),
        }[k]
        return self.remote(k, src, dst, rel)

    def gather_copy(self, k):
        n = self.half
        src_rel, lo, cnt, to, from_res = {
            10: (0, 0, n, XN, True), 11: (0, n, n, XN, True),
            12: (0, n, n, YN, True), 13: (0, 0, n, YN, True),
            14: (0, 0, 2 * n, CORE, True),
            15: (YN, n, n, XN, False), 16: (XN, 0, n, YN, False),
            17: (XN, 0, n, CORE, False), 18: (XN, n, n, CORE, False),
            19: (YN, n, n, CORE, False), 20: (YN, 0, n, CORE, False),
            21: (DIAG, n, n, CORE, False), 22: (DIAG, 0, n, CORE, False),
        }[k]
        dst = self.full.at[self.block(src_rel, self.row0, lo, cnt)]
        return self.remote(k, self.res.at[pl.ds(lo, cnt)] if from_res else dst, dst, to)

    def keep_copy(self):
        return self.local(6, self.res, self.full.at[self.block(0, self.row0)])

    def start(self):
        for j in range(4):
            self.core_copy(j).start()
            self.local_copy(j).start()
        self.side_copy(0).start()
        if self.base is not None:
            self.side_copy(1).start()

    def add(self, dst, src):
        @pl.loop(0, dst.shape[0] // 16)
        def _(i):
            r = pl.ds(pl.multiple_of(i * 16, 16), 16)
            dst[r, :] = (dst[r, :].astype(F32) + src[r, :].astype(F32)).astype(BF16)

    def chip_sums(self):
        for j in range(4):
            self.local_copy(j).wait()
            self.core_copy(j).wait_recv()
            self.add(self.sums.at[j], self.from_core.at[j])
            for k in {0: (4, 5), 1: (6,), 2: (7,), 3: ()}[j]:
                self.scatter_copy(k).start()
        for j in range(4):
            self.core_copy(j).wait_send()

    def forward_sums(self):
        lo, hi = pl.ds(0, self.half), pl.ds(self.half, self.half)
        self.scatter_copy(5).wait_recv()
        self.add(self.sums.at[1, hi], self.via.at[1])
        self.scatter_copy(8).start()
        self.scatter_copy(4).wait_recv()
        self.add(self.sums.at[2, lo], self.via.at[0])
        self.scatter_copy(9).start()

    def norm_and_send(self):
        for k in (6, 7, 8, 9):
            self.scatter_copy(k).wait_recv()
        self.side_copy(0).wait()
        first = self.base is not None
        if first:
            self.side_copy(1).wait()
        gain = self.gain[...].astype(F32)
        base = self.me * self.rows + self.row0

        @pl.loop(0, self.rows // 16)
        def _(i):
            r = pl.ds(pl.multiple_of(i * 16, 16), 16)
            g = pl.ds(pl.multiple_of(base + i * 16, 16), 16)
            mean = self.st[g, self.st_col:self.st_col + 1]
            rstd = self.st[g, self.st_col + 1:self.st_col + 2]
            grad = self.sums[3, r, :].astype(F32) + self.mine[0, r, :].astype(F32) + self.mine[1, r, :].astype(F32)
            zh = (self.zv[r, :].astype(F32) - mean) * rstd
            u = grad * gain
            mean_u = jnp.mean(u, axis=1, keepdims=True)
            mean_p = jnp.mean(u * zh, axis=1, keepdims=True)
            added = self.bv[r, :].astype(F32) if first else self.resf[r, :]
            out = added + rstd * (u - mean_u - zh * mean_p)
            if first:
                self.resf[r, :] = out
            self.res[r, :] = out.astype(BF16)
        for k in (10, 12, 11, 13, 14):
            self.gather_copy(k).start()
        self.keep_copy().start()

    def forward_first(self):
        self.gather_copy(10).wait_recv()
        self.gather_copy(16).start()
        self.gather_copy(12).wait_recv()
        self.gather_copy(15).start()
        self.gather_copy(17).start()
        self.gather_copy(19).start()

    def forward_second(self):
        self.gather_copy(11).wait_recv()
        self.gather_copy(18).start()
        self.gather_copy(13).wait_recv()
        self.gather_copy(20).start()

    def finish(self):
        self.gather_copy(15).wait_recv()
        self.gather_copy(21).start()
        self.gather_copy(16).wait_recv()
        self.gather_copy(22).start()
        for k in (14, 17, 18, 19, 20, 21, 22):
            self.gather_copy(k).wait_recv()
        for k in range(4, 10):
            self.scatter_copy(k).wait_send()
        for k in range(10, 23):
            self.gather_copy(k).wait_send()
        self.keep_copy().wait()

    def events(self):
        return [self.start, self.chip_sums, self.forward_sums, self.norm_and_send, self.forward_first,
                self.forward_second, self.finish]


class Timeline:
    def __init__(self, events):
        self.now = 0.0
        self.events = sorted(events, key=lambda e: e[0])

    def take(self, until):
        due = [e for e in self.events if e[0] < until]
        self.events = self.events[len(due):]
        return due

    def pipeline(self, body, steps, us, in_specs, out_specs, refs):
        here = [(max(0, int((t - self.now) / us)), e) for t, e in self.take(self.now + steps * us)]

        def step(*tiles):
            for w, e in here:
                pl.when(pl.program_id(0) == w)(e)
            body(*tiles)

        pltpu.emit_pipeline(step, grid=(steps,), in_specs=in_specs, out_specs=out_specs)(*refs)
        self.now += steps * us

    def piece(self, us, fn):
        for _, e in self.take(self.now + us / 2):
            e()
        fn()
        self.now += us

    def drain(self):
        for _, e in self.take(float("inf")):
            e()


def rows_spec(n, w, first=0):
    return pl.BlockSpec((n, w), lambda i: (i + first, 0))


def cols_spec(h, n, first=0):
    return pl.BlockSpec((h, n), lambda i: (0, i + first))


def attend(qkv_ref, do_ref, do_row, o_ref, dqkv_ref, dk_acc, dv_acc, c, h, chunk, group, hd):
    scale = hd ** -0.5
    kv = (c + 1) * chunk
    mine = slice(c * chunk, kv)
    cols = slice(h * hd, (h + 1) * hd)
    keys = qkv_ref[0:kv, group * hd:(group + 1) * hd]
    vals = qkv_ref[0:kv, (group + 1) * hd:(group + 2) * hd]
    q_pos = c * chunk + lax.broadcasted_iota(jnp.int32, (chunk, kv), 0)
    causal = q_pos >= lax.broadcasted_iota(jnp.int32, (chunk, kv), 1)
    q = qkv_ref[mine, cols]
    do = do_ref[do_row:do_row + chunk, cols]
    s = jnp.where(causal, dot(q, keys, 1, 1) * scale, -1e30)
    e = jnp.exp(s - jnp.max(s, axis=1, keepdims=True))
    p = e * (1.0 / jnp.sum(e, axis=1, keepdims=True))
    p_low = p.astype(BF16)
    o_ref[mine, cols] = dot(p_low, vals, 1, 0).astype(BF16)
    dp = dot(do, vals, 1, 1)
    row_dot = jnp.sum(p * dp, axis=1, keepdims=True)
    ds = (p * (dp - row_dot) * scale).astype(BF16)
    dqkv_ref[mine, cols] = dot(ds, keys, 1, 0).astype(BF16)
    dk_acc[:, 0:kv] += dot(q, ds, 0, 0)
    dv_acc[:, 0:kv] += dot(do, p_low, 0, 0)


def layer_body(part, h, d_out, st, gain_h, gain_x, n, hid_up, dg_up, du_up, wg, wu, wd, x, wqkv, wo,
               dmid, dx, dwg, dwu, nx, hid, o, dqkv,
               hidv, dgv, duv, qkvv, dqv, ov, dov, dmv, pxv, wov, dk_acc, dv_acc, wsem, lsem, ssem, rsem,
               *scratch, rows, hd):
    t, d = h.shape
    f = wg.shape[1]
    c = wqkv.shape[1]
    group = c // hd - 2
    t2 = t // 2
    half = len(scratch) // 2
    sc_up, sc_lo = scratch[:half], scratch[half:]
    sems = (lsem, ssem, rsem)
    ex = [
        Exchange(0, rows, t2, part, 0, h, d_out, st, 0, gain_h, dmid, sc_up, sems),
        Exchange(1, rows, 0, pxv, 0, h, d_out, st, 0, gain_h, dmid, sc_lo, sems),
        Exchange(2, rows, t2, pxv, 0, x, None, st, 2, gain_x, dx, sc_up, sems),
        Exchange(3, rows, 0, pxv, 0, x, None, st, 2, gain_x, dx, sc_lo, sems),
    ]
    copy = lambda i, s, v: pltpu.make_async_copy(s, v, wsem.at[i])
    n_lo = copy(0, n.at[pl.ds(0, t2)], dmv)
    do_lo = copy(1, d_out.at[pl.ds(0, t2)], wov)
    ups = [copy(2 + i, s, v.at[pl.ds(t2, t2)]) for i, (s, v) in enumerate(((hid_up, hidv), (dg_up, dgv), (du_up, duv)))]
    load_wo = copy(1, wo, wov)
    load_dm = [copy(6, dmid.at[pl.ds(0, t2)], dmv), copy(6, dmid.at[pl.ds(t2, t2)], dmv)]
    keep_hid, keep_o, keep_dqkv = copy(7, hidv, hid), copy(8, ov, o), copy(9, dqv, dqkv)

    n_lo.start()
    do_lo.start()
    barrier = pltpu.get_barrier_semaphore()
    for rel in (CORE, XN, YN):
        pl.semaphore_signal(barrier, inc=1, device_id={"tp": ex[0].peer(rel)}, device_id_type=pl.DeviceIdType.MESH)
    pl.semaphore_wait(barrier, 3)
    ex[0].start()
    for u in ups:
        u.start()
    dk_acc[...] = jnp.zeros_like(dk_acc)
    dv_acc[...] = jnp.zeros_like(dv_acc)

    def finish_first(e, which):
        def run():
            ex[e].finish()
            load_dm[which].start()
        return run

    times = [
        list(zip((4, 13, 22, 31, 35), ex[0].events()[1:6])) + [(50.5, finish_first(0, 1))],
        list(zip((50, 54, 61, 72, 80, 85), ex[1].events()[:6])) + [(90.5, finish_first(1, 0))],
        list(zip((79, 83, 98, 110, 121, 129, 140), ex[2].events())),
        list(zip((104, 108, 122, 141, 150, 155, 160), ex[3].events())),
    ]
    tl = Timeline(sum(times, []))
    n_lo.wait()
    do_lo.wait()
    lower = slice(0, t2)

    def mlp(wg_t, wu_t, wd_t):
        col = pl.ds(pl.multiple_of(pl.program_id(0) * 256, 256), 256)
        hidv[lower, col], dgv[lower, col], duv[lower, col] = swiglu_grads(dmv[...], wov[...], wg_t[...], wu_t[...], wd_t[...])

    tl.pipeline(mlp, f // 256, 31 / 7, [cols_spec(d, 256), cols_spec(d, 256), rows_spec(256, d)], [], (wg, wu, wd))
    load_wo.start()
    for u in ups:
        u.wait()
    keep_hid.start()

    def rest(wv):
        load_wqkv = copy(5, wqkv, wv)
        load_wqkv.start()

        def part_lo(wg_t, wu_t):
            col = pl.ds(pl.multiple_of(pl.program_id(0) * 512, 512), 512)
            pxv[:, col] = (dot(dgv[lower, :], wg_t[...], 1, 1) + dot(duv[lower, :], wu_t[...], 1, 1)).astype(BF16)

        tl.pipeline(part_lo, d // 512, 19 / 8, [rows_spec(512, f)] * 2, [], (wg, wu))
        load_wqkv.wait()
        load_wo.wait()
        rb = 128

        def project(x_t, n_t):
            r = pl.ds(pl.multiple_of(pl.program_id(0) * rb, rb), rb)
            n_t[...] = normed(x_t[...], st[r, 2:3], st[r, 3:4], gain_x[...])
            qkvv[r, :] = dot(n_t[...], wv[...], 1, 0).astype(BF16)

        tl.pipeline(project, t // rb, 10.5 / 8, [rows_spec(rb, d)], [rows_spec(rb, d)], (x, nx))

        def attention_half(which, us):
            lo = which * t2
            chunk = t2 // 2

            def heads():
                load_dm[which].wait()
                dov[...] = dot(dmv[...], wov[...], 1, 1).astype(BF16)

            tl.piece(2.5, heads)
            for cc in (2 * which + 1, 2 * which):
                for g in range(group):
                    def one(cc=cc, g=g):
                        attend(qkvv, dov, cc * chunk - lo, ov, dqv, dk_acc, dv_acc, cc, g, chunk, group, hd)
                    tl.piece(us * (cc + 1), one)

            def project_back():
                mine = slice(lo, lo + t2)
                dqv[mine, group * hd:(group + 1) * hd] = dk_acc[:, mine].T.astype(BF16)
                dqv[mine, (group + 1) * hd:(group + 2) * hd] = dv_acc[:, mine].T.astype(BF16)
                for j in range(d // 512):
                    col = slice(j * 512, (j + 1) * 512)
                    pxv[:, col] = dot(dqv[mine, :], wv[col, :], 1, 1).astype(BF16)

            tl.piece(4, project_back)

        def weight_grads(n_t, g_t, u_t):
            g_t[...] = dot(n_t[...], dgv[...], 0, 0).astype(BF16)
            u_t[...] = dot(n_t[...], duv[...], 0, 0).astype(BF16)

        def weights(first, steps):
            tl.pipeline(weight_grads, steps, 2.4, [cols_spec(t, 256, first)], [rows_spec(256, f, first)] * 2, (n, dwg, dwu))

        attention_half(1, 0.45)
        weights(0, 5)
        attention_half(0, 0.45)
        keep_o.start()
        keep_dqkv.start()
        weights(5, d // 256 - 5)
        tl.drain()

    pl.run_scoped(rest, pltpu.VMEM((d, c), BF16))
    keep_hid.wait()
    keep_o.wait()
    keep_dqkv.wait()


def layer(part, h, d_out, stats, gain_h, gain_x, n, hid_up, dg_up, du_up, wg, wu, wd, x, wqkv, wo, hd, tp):
    t, d = h.shape
    f = wg.shape[1]
    c = wqkv.shape[1]
    hw = wo.shape[0]
    rows = t // 2 // tp
    vm = lambda a, b, dt=BF16: pltpu.VMEM((a, b), dt)
    return pl.pallas_call(
        functools.partial(layer_body, rows=rows, hd=hd),
        in_specs=[ANY, ANY, ANY, IN_VMEM, IN_VMEM, IN_VMEM] + [ANY] * 10,
        out_specs=[ANY] * 8,
        out_shape=[shape_of((t, d)), shape_of((t, d)), shape_of((d, f)), shape_of((d, f)), shape_of((t, d)),
                   shape_of((t, f)), shape_of((t, hw)), shape_of((t, c))],
        scratch_shapes=[vm(t, f), vm(t, f), vm(t, f), vm(t, c), vm(t, c), vm(t, hw), vm(t // 2, hw),
                        vm(t // 2, d), vm(t // 2, d), vm(hw, d), vm(hd, t, F32), vm(hd, t, F32),
                        pltpu.SemaphoreType.DMA((10,)), pltpu.SemaphoreType.DMA((32,)),
                        pltpu.SemaphoreType.DMA((4 * COPIES,)), pltpu.SemaphoreType.DMA((4 * COPIES,))]
        + exchange_scratch(rows, d) * 2,
        compiler_params=pltpu.CompilerParams(vmem_limit_bytes=67043328, collective_id=1, has_side_effects=True),
        name="layer",
    )(part, h, d_out, stats, gain_h, gain_x, n, hid_up, dg_up, du_up, wg, wu, wd, x, wqkv, wo)


def last_body(do_ref, hid_ref, nx_ref, dqkv_ref, dm_ref, o_ref, dwg_in, dwu_in, dx_in,
              dwd_ref, dwqkv_ref, dwo_ref, dwg_ref, dwu_ref, dx_ref):
    dwg_ref[...] = dwg_in[...]
    dwu_ref[...] = dwu_in[...]
    dx_ref[...] = dx_in[...]
    dwd_ref[...] = dot(hid_ref[...], do_ref[...], 0, 0).astype(BF16)
    dwqkv_ref[...] = dot(nx_ref[...], dqkv_ref[...], 0, 0).astype(BF16)
    dwo_ref[...] = dot(o_ref[...], dm_ref[...], 0, 0).astype(BF16)


def last(d_out, hid, nx, dqkv, dmid, o, dwg, dwu, dx, block=512):
    t, d = d_out.shape
    f, c, hw = hid.shape[1], dqkv.shape[1], o.shape[1]
    steps = d // block
    moved = [rows_spec(block, f), rows_spec(block, f), rows_spec(t // steps, d)]
    return pl.pallas_call(
        last_body,
        grid=(steps,),
        in_specs=[cols_spec(t, block), resident((t, f)), cols_spec(t, block), resident((t, c)), cols_spec(t, block),
                  resident((t, hw))] + moved,
        out_specs=[cols_spec(f, block), rows_spec(block, c), cols_spec(hw, block)] + moved,
        out_shape=[shape_of((f, d)), shape_of((d, c)), shape_of((hw, d)), shape_of((d, f)), shape_of((d, f)), shape_of((t, d))],
        compiler_params=params(),
        name="last",
    )(d_out, hid, nx, dqkv, dmid, o, dwg, dwu, dx)


def solution(mesh):
    tp = mesh.shape["tp"]

    def device_step(x_in, h_mid, mean_x, rstd_x, mean_h, rstd_h, gain_x, gain_h, w_qkv, w_out, w_gate, w_up, w_down, d_out):
        heads, hd, d = w_out.shape
        stats = jnp.stack([mean_h, rstd_h, mean_x, rstd_x], axis=1)
        gx, gh = gain_x.reshape(1, d), gain_h.reshape(1, d)
        hid_up, dg_up, du_up, norm_h = mlp_grads(h_mid, stats, gh, d_out, w_gate, w_up, w_down)
        part = mlp_part(dg_up, du_up, w_gate, w_up)
        d_mid, d_x, d_w_gate, d_w_up, norm_x, hid, o, d_qkv = layer(
            part, h_mid, d_out, stats, gh, gx, norm_h, hid_up, dg_up, du_up, w_gate, w_up, w_down, x_in, w_qkv,
            w_out.reshape(heads * hd, d), hd, tp)
        d_w_down, d_w_qkv, d_w_out, d_w_gate, d_w_up, d_x = last(
            d_out, hid, norm_x, d_qkv, d_mid, o, d_w_gate, d_w_up, d_x)
        return d_x, d_w_qkv, d_w_out.reshape(w_out.shape), d_w_gate, d_w_up, d_w_down

    row_spec = P('dp', None)
    stat_spec = P('dp')
    col_spec = P(None, 'tp')
    in_specs = (row_spec, row_spec, stat_spec, stat_spec, stat_spec, stat_spec, P(None), P(None), col_spec, P('tp', None, None), col_spec, col_spec, P('tp', None), row_spec)
    out_specs = (row_spec, P('dp', 'tp'), P(('dp', 'tp'), None, None), P('dp', 'tp'), P('dp', 'tp'), P(('dp', 'tp'), None))
    return jax.shard_map(device_step, mesh=mesh, in_specs=in_specs, out_specs=out_specs, check_vma=False)
```

```python
import functools

import jax
import jax.numpy as jnp
from jax import lax
from jax.experimental import pallas as pl
from jax.experimental.pallas import tpu as pltpu
from jax.sharding import PartitionSpec as P

F32 = jnp.float32
BF16 = jnp.bfloat16
VMEM_LIMIT = 62 * 1024 * 1024
ANY = pl.BlockSpec(memory_space=pl.ANY)
IN_VMEM = pl.BlockSpec(memory_space=pltpu.VMEM)


def dot(lhs, rhs, lhs_dim, rhs_dim):
    return lax.dot_general(lhs, rhs, (((lhs_dim,), (rhs_dim,)), ((), ())), preferred_element_type=F32)


def resident(shape):
    return pl.BlockSpec(shape, lambda i: (0,) * len(shape), pipeline_mode=pl.Buffered(1))


def shape_of(shape, dtype=BF16):
    return jax.ShapeDtypeStruct(shape, dtype)


def params(**kw):
    return pltpu.CompilerParams(vmem_limit_bytes=VMEM_LIMIT, **kw)


def normed(src, mean, rstd, gain):
    return (((src.astype(F32) - mean) * rstd) * gain).astype(BF16)


def swiglu_grads(n, d_out, wg, wu, wd):
    gate = dot(n, wg, 1, 0).astype(BF16).astype(F32)
    up = dot(n, wu, 1, 0).astype(BF16).astype(F32)
    d_hid = dot(d_out, wd, 1, 1).astype(BF16).astype(F32)
    sig = jax.nn.sigmoid(gate)
    act = gate * sig
    return ((act * up).astype(BF16), (d_hid * up * sig * (1.0 + gate * (1.0 - sig))).astype(BF16),
            (d_hid * act).astype(BF16))


def mlp_body(h_ref, st_ref, gain_ref, do_ref, wg_ref, wu_ref, wd_ref, hid_ref, dg_ref, du_ref, n_ref):
    rows = h_ref.shape[0]
    upper = slice(rows // 2, rows)

    @pl.when(pl.program_id(0) == 0)
    def _():
        @pl.loop(0, rows // 128)
        def _(i):
            r = pl.ds(pl.multiple_of(i * 128, 128), 128)
            n_ref[r, :] = normed(h_ref[r, :], st_ref[r, 0:1], st_ref[r, 1:2], gain_ref[0:1, :])

    hid_ref[...], dg_ref[...], du_ref[...] = swiglu_grads(n_ref[upper, :], do_ref[...], wg_ref[...], wu_ref[...], wd_ref[...])


def mlp_grads(h, stats, gain, d_out, wg, wu, wd, block=256):
    t, d = h.shape
    f = wg.shape[1]
    col = lambda n: pl.BlockSpec((n, block), lambda i: (0, i))
    return pl.pallas_call(
        mlp_body,
        grid=(f // block,),
        in_specs=[resident((t, d)), resident(stats.shape), resident(gain.shape), pl.BlockSpec((t // 2, d), lambda i: (1, 0), pipeline_mode=pl.Buffered(1)),
                  col(d), col(d), pl.BlockSpec((block, d), lambda i: (i, 0))],
        out_specs=[col(t // 2)] * 3 + [resident((t, d))],
        out_shape=[shape_of((t // 2, f))] * 3 + [shape_of((t, d))],
        compiler_params=params(),
        name="mlp_grads",
    )(h, stats, gain, d_out, wg, wu, wd)


def part_body(dg_ref, du_ref, wg_ref, wu_ref, out_ref):
    out_ref[...] = (dot(dg_ref[...], wg_ref[...], 1, 1) + dot(du_ref[...], wu_ref[...], 1, 1)).astype(BF16)


def mlp_part(dg, du, wg, wu, block=512):
    t, f = dg.shape
    d = wg.shape[0]
    return pl.pallas_call(
        part_body,
        grid=(d // block,),
        in_specs=[resident((t, f)), resident((t, f))] + [pl.BlockSpec((block, f), lambda i: (i, 0))] * 2,
        out_specs=pl.BlockSpec((t, block), lambda i: (0, i)),
        out_shape=shape_of((t, d)),
        compiler_params=params(),
        name="mlp_part",
    )(dg, du, wg, wu)


CORE, XN, YN, DIAG = 1, 2, 4, 6
ORDER = (DIAG, XN, YN, 0)
COPIES = 24


def exchange_scratch(rows, d):
    half = rows // 2
    return [
        pltpu.VMEM((4, rows, d), BF16),
        pltpu.VMEM((4, rows, d), BF16),
        pltpu.VMEM((2, half, d), BF16),
        pltpu.VMEM((2, rows, d), BF16),
        pltpu.VMEM((rows, d), BF16),
        pltpu.VMEM((rows, d), BF16),
        pltpu.VMEM((rows, d), BF16),
        pltpu.VMEM((rows, d), F32),
    ]


class Exchange:
    def __init__(self, index, rows, row0, part, part0, z, base, st, st_col, gain, full, scratch, sems):
        self.index, self.rows, self.half, self.row0 = index, rows, rows // 2, row0
        self.part, self.part0, self.z, self.base = part, part0, z, base
        self.st, self.st_col, self.gain, self.full = st, st_col, gain, full
        self.from_core, self.sums, self.via, self.mine, self.res, self.zv, self.bv, self.resf = scratch
        self.lsem, self.ssem, self.rsem = sems
        self.me = lax.axis_index("tp")

    def peer(self, rel):
        return lax.bitwise_xor(self.me, rel)

    def block(self, rel, base, lo=0, n=None):
        n = self.rows if n is None else n
        return pl.ds(pl.multiple_of(self.peer(rel) * self.rows + base + lo, 16), n)

    def remote(self, k, src, dst, rel):
        k = self.index * COPIES + k
        return pltpu.make_async_remote_copy(
            src_ref=src, dst_ref=dst, send_sem=self.ssem.at[k], recv_sem=self.rsem.at[k],
            device_id={"tp": self.peer(rel)}, device_id_type=pl.DeviceIdType.MESH)

    def local(self, k, src, dst):
        return pltpu.make_async_copy(src, dst, self.lsem.at[self.index * 8 + k])

    def core_copy(self, j):
        return self.remote(j, self.part.at[self.block(ORDER[j] ^ CORE, self.part0)], self.from_core.at[j], CORE)

    def local_copy(self, j):
        return self.local(j, self.part.at[self.block(ORDER[j], self.part0)], self.sums.at[j])

    def side_copy(self, k):
        if k == 0:
            return self.local(4, self.z.at[self.block(0, self.row0)], self.zv)
        return self.local(5, self.base.at[self.block(0, self.row0)], self.bv)

    def scatter_copy(self, k):
        lo, hi = pl.ds(0, self.half), pl.ds(self.half, self.half)
        src, dst, rel = {
            4: (self.sums.at[0, lo], self.via.at[0], XN),
            5: (self.sums.at[0, hi], self.via.at[1], YN),
            6: (self.sums.at[1, lo], self.mine.at[0, lo], XN),
            7: (self.sums.at[2, hi], self.mine.at[1, hi], YN),
            8: (self.sums.at[1, hi], self.mine.at[0, hi], XN),
            9: (self.sums.at[2, lo], self.mine.at[1, lo], YN),
        }[k]
        return self.remote(k, src, dst, rel)

    def gather_copy(self, k):
        n = self.half
        src_rel, lo, cnt, to, from_res = {
            10: (0, 0, n, XN, True), 11: (0, n, n, XN, True),
            12: (0, n, n, YN, True), 13: (0, 0, n, YN, True),
            14: (0, 0, 2 * n, CORE, True),
            15: (YN, n, n, XN, False), 16: (XN, 0, n, YN, False),
            17: (XN, 0, n, CORE, False), 18: (XN, n, n, CORE, False),
            19: (YN, n, n, CORE, False), 20: (YN, 0, n, CORE, False),
            21: (DIAG, n, n, CORE, False), 22: (DIAG, 0, n, CORE, False),
        }[k]
        dst = self.full.at[self.block(src_rel, self.row0, lo, cnt)]
        return self.remote(k, self.res.at[pl.ds(lo, cnt)] if from_res else dst, dst, to)

    def keep_copy(self):
        return self.local(6, self.res, self.full.at[self.block(0, self.row0)])

    def start(self):
        for j in range(4):
            self.core_copy(j).start()
            self.local_copy(j).start()
        self.side_copy(0).start()
        if self.base is not None:
            self.side_copy(1).start()

    def add(self, dst, src):
        @pl.loop(0, dst.shape[0] // 16)
        def _(i):
            r = pl.ds(pl.multiple_of(i * 16, 16), 16)
            dst[r, :] = (dst[r, :].astype(F32) + src[r, :].astype(F32)).astype(BF16)

    def chip_sums(self):
        for j in range(4):
            self.local_copy(j).wait()
            self.core_copy(j).wait_recv()
            self.add(self.sums.at[j], self.from_core.at[j])
            for k in {0: (4, 5), 1: (6,), 2: (7,), 3: ()}[j]:
                self.scatter_copy(k).start()
        for j in range(4):
            self.core_copy(j).wait_send()

    def forward_sums(self):
        lo, hi = pl.ds(0, self.half), pl.ds(self.half, self.half)
        self.scatter_copy(5).wait_recv()
        self.add(self.sums.at[1, hi], self.via.at[1])
        self.scatter_copy(8).start()
        self.scatter_copy(4).wait_recv()
        self.add(self.sums.at[2, lo], self.via.at[0])
        self.scatter_copy(9).start()

    def norm_and_send(self):
        for k in (6, 7, 8, 9):
            self.scatter_copy(k).wait_recv()
        self.side_copy(0).wait()
        first = self.base is not None
        if first:
            self.side_copy(1).wait()
        gain = self.gain[...]
        base = self.me * self.rows + self.row0

        @pl.loop(0, self.rows // 16)
        def _(i):
            r = pl.ds(pl.multiple_of(i * 16, 16), 16)
            g = pl.ds(pl.multiple_of(base + i * 16, 16), 16)
            mean = self.st[g, self.st_col:self.st_col + 1]
            rstd = self.st[g, self.st_col + 1:self.st_col + 2]
            grad = self.sums[3, r, :].astype(F32) + self.mine[0, r, :].astype(F32) + self.mine[1, r, :].astype(F32)
            zh = (self.zv[r, :].astype(F32) - mean) * rstd
            u = grad * gain
            mean_u = jnp.mean(u, axis=1, keepdims=True)
            mean_p = jnp.mean(u * zh, axis=1, keepdims=True)
            added = self.bv[r, :].astype(F32) if first else self.resf[r, :]
            out = added + rstd * (u - mean_u - zh * mean_p)
            if first:
                self.resf[r, :] = out
            self.res[r, :] = out.astype(BF16)
        for k in (10, 12, 11, 13, 14):
            self.gather_copy(k).start()
        self.keep_copy().start()

    def forward_first(self):
        self.gather_copy(10).wait_recv()
        self.gather_copy(16).start()
        self.gather_copy(12).wait_recv()
        self.gather_copy(15).start()
        self.gather_copy(17).start()
        self.gather_copy(19).start()

    def forward_second(self):
        self.gather_copy(11).wait_recv()
        self.gather_copy(18).start()
        self.gather_copy(13).wait_recv()
        self.gather_copy(20).start()

    def finish(self):
        self.gather_copy(15).wait_recv()
        self.gather_copy(21).start()
        self.gather_copy(16).wait_recv()
        self.gather_copy(22).start()
        for k in (14, 17, 18, 19, 20, 21, 22):
            self.gather_copy(k).wait_recv()
        for k in range(4, 10):
            self.scatter_copy(k).wait_send()
        for k in range(10, 23):
            self.gather_copy(k).wait_send()
        self.keep_copy().wait()

    def events(self):
        return [self.start, self.chip_sums, self.forward_sums, self.norm_and_send, self.forward_first,
                self.forward_second, self.finish]


class Timeline:
    def __init__(self, events):
        self.now = 0.0
        self.events = sorted(events, key=lambda e: e[0])

    def take(self, until):
        due = [e for e in self.events if e[0] < until]
        self.events = self.events[len(due):]
        return due

    def pipeline(self, body, steps, us, in_specs, out_specs, refs):
        here = [(max(0, int((t - self.now) / us)), e) for t, e in self.take(self.now + steps * us)]

        def step(*tiles):
            for w, e in here:
                pl.when(pl.program_id(0) == w)(e)
            body(*tiles)

        pltpu.emit_pipeline(step, grid=(steps,), in_specs=in_specs, out_specs=out_specs)(*refs)
        self.now += steps * us

    def loop(self, fn, steps, us):
        here = [(max(0, int((t - self.now) / us)), e) for t, e in self.take(self.now + steps * us)]

        @pl.loop(0, steps)
        def _(i):
            for w, e in here:
                pl.when(i == w)(e)
            fn(i)

        self.now += steps * us

    def piece(self, us, fn):
        for _, e in self.take(self.now + us / 2):
            e()
        fn()
        self.now += us

    def drain(self):
        for _, e in self.take(float("inf")):
            e()


def rows_spec(n, w, first=0):
    return pl.BlockSpec((n, w), lambda i: (i + first, 0))


def cols_spec(h, n, first=0):
    return pl.BlockSpec((h, n), lambda i: (0, i + first))


def attend(qkv_ref, do_ref, do_row, o_ref, dqkv_ref, dk_acc, dv_acc, c, h, chunk, group, hd):
    scale = hd ** -0.5
    kv = (c + 1) * chunk
    mine = slice(c * chunk, kv)
    cols = pl.ds(pl.multiple_of(h * hd, hd), hd)
    keys = qkv_ref[0:kv, group * hd:(group + 1) * hd]
    vals = qkv_ref[0:kv, (group + 1) * hd:(group + 2) * hd]
    q_pos = c * chunk + lax.broadcasted_iota(jnp.int32, (chunk, kv), 0)
    causal = q_pos >= lax.broadcasted_iota(jnp.int32, (chunk, kv), 1)
    q = qkv_ref[mine, cols]
    do = do_ref[do_row:do_row + chunk, cols]
    s = jnp.where(causal, dot(q, keys, 1, 1) * scale, -1e30)
    e = jnp.exp(s - jnp.max(s, axis=1, keepdims=True))
    p = e * (1.0 / jnp.sum(e, axis=1, keepdims=True))
    p_low = p.astype(BF16)
    o_ref[mine, cols] = dot(p_low, vals, 1, 0).astype(BF16)
    dp = dot(do, vals, 1, 1)
    row_dot = jnp.sum(p * dp, axis=1, keepdims=True)
    ds = (p * (dp - row_dot) * scale).astype(BF16)
    dqkv_ref[mine, cols] = dot(ds, keys, 1, 0).astype(BF16)
    dk_acc[:, 0:kv] += dot(q, ds, 0, 0)
    dv_acc[:, 0:kv] += dot(do, p_low, 0, 0)


def layer_body(part, h, d_out, st, gains, n, hid_up, dg_up, du_up, wg, wu, wd, x, wqkv, wo,
               dmid, dx, dwg, dwu, nx, dwd, o, dqkv,
               hidv, dgv, duv, qkvv, dqv, ov, dov, dmv, pxv, wov, dk_acc, dv_acc, wsem, lsem, ssem, rsem,
               *scratch, rows, hd):
    t, d = h.shape
    f = wg.shape[1]
    c = wqkv.shape[1]
    group = c // hd - 2
    t2 = t // 2
    half = len(scratch) // 2
    sc_up, sc_lo = scratch[:half], scratch[half:]
    sems = (lsem, ssem, rsem)
    ex = [
        Exchange(0, rows, t2, part, 0, h, d_out, st, 0, gains.at[0:1], dmid, sc_up, sems),
        Exchange(1, rows, 0, pxv, 0, h, d_out, st, 0, gains.at[0:1], dmid, sc_lo, sems),
        Exchange(2, rows, t2, pxv, 0, x, None, st, 2, gains.at[1:2], dx, sc_up, sems),
        Exchange(3, rows, 0, pxv, 0, x, None, st, 2, gains.at[1:2], dx, sc_lo, sems),
    ]
    copy = lambda i, s, v: pltpu.make_async_copy(s, v, wsem.at[i])
    n_lo = copy(0, n.at[pl.ds(0, t2)], dmv)
    do_lo = copy(1, d_out.at[pl.ds(0, t2)], wov)
    ups = [copy(2 + i, s, v.at[pl.ds(t2, t2)]) for i, (s, v) in enumerate(((hid_up, hidv), (dg_up, dgv), (du_up, duv)))]
    load_wo = copy(1, wo, wov)
    load_dm = [copy(6, dmid.at[pl.ds(0, t2)], dmv), copy(6, dmid.at[pl.ds(t2, t2)], dmv)]

    keep_o, keep_dqkv = copy(8, ov, o), copy(9, dqv, dqkv)

    n_lo.start()
    do_lo.start()
    barrier = pltpu.get_barrier_semaphore()
    for rel in (CORE, XN, YN):
        pl.semaphore_signal(barrier, inc=1, device_id={"tp": ex[0].peer(rel)}, device_id_type=pl.DeviceIdType.MESH)
    pl.semaphore_wait(barrier, 3)
    ex[0].start()
    for u in ups:
        u.start()
    dk_acc[...] = jnp.zeros_like(dk_acc)
    dv_acc[...] = jnp.zeros_like(dv_acc)

    def finish_first(e, which):
        def run():
            ex[e].finish()
            load_dm[which].start()
        return run

    times = [
        list(zip((5, 13, 26, 36, 42), ex[0].events()[1:6])) + [(52, finish_first(0, 1))],
        list(zip((49.1, 53, 60, 71, 80, 86), ex[1].events()[:6])) + [(92, finish_first(1, 0))],
        list(zip((76.2, 84, 94, 102, 107, 112, 120), ex[2].events())),
        list(zip((108, 111, 118, 127, 136, 141, 148), ex[3].events())),
    ]
    tl = Timeline(sum(times, []))
    n_lo.wait()
    do_lo.wait()
    lower = slice(0, t2)

    def mlp(wg_t, wu_t, wd_t):
        col = pl.ds(pl.multiple_of(pl.program_id(0) * 256, 256), 256)
        hidv[lower, col], dgv[lower, col], duv[lower, col] = swiglu_grads(dmv[...], wov[...], wg_t[...], wu_t[...], wd_t[...])

    tl.pipeline(mlp, f // 256, 30 / 7, [cols_spec(d, 256), cols_spec(d, 256), rows_spec(256, d)], [], (wg, wu, wd))
    load_wo.start()
    for u in ups:
        u.wait()

    def rest(wv):
        load_wqkv = copy(5, wqkv, wv)
        load_wqkv.start()

        def part_lo(wg_t, wu_t):
            col = pl.ds(pl.multiple_of(pl.program_id(0) * 512, 512), 512)
            pxv[:, col] = (dot(dgv[lower, :], wg_t[...], 1, 1) + dot(duv[lower, :], wu_t[...], 1, 1)).astype(BF16)

        tl.pipeline(part_lo, d // 512, 19 / 8, [rows_spec(512, f)] * 2, [], (wg, wu))
        load_wqkv.wait()
        load_wo.wait()
        rb = 128

        def project(x_t, n_t):
            r = pl.ds(pl.multiple_of(pl.program_id(0) * rb, rb), rb)
            n_t[...] = normed(x_t[...], st[r, 2:3], st[r, 3:4], gains[1:2, :])
            qkvv[r, :] = dot(n_t[...], wv[...], 1, 0).astype(BF16)

        tl.pipeline(project, t // rb, 10 / 8, [rows_spec(rb, d)], [rows_spec(rb, d)], (x, nx))

        def attention_half(which, us):
            lo = which * t2
            chunk = t2 // 2

            def heads():
                load_dm[which].wait()
                dov[...] = dot(dmv[...], wov[...], 1, 1).astype(BF16)

            tl.piece(2.5, heads)
            for cc in (2 * which + 1, 2 * which):
                def one(g, cc=cc):
                    attend(qkvv, dov, cc * chunk - lo, ov, dqv, dk_acc, dv_acc, cc, g, chunk, group, hd)
                tl.loop(one, group, us * (cc + 1))

            mine = slice(lo, lo + t2)

            def key_grads():
                dqv[mine, group * hd:(group + 1) * hd] = dk_acc[:, mine].T.astype(BF16)
                dqv[mine, (group + 1) * hd:(group + 2) * hd] = dv_acc[:, mine].T.astype(BF16)

            def project_back(j):
                col = pl.ds(pl.multiple_of(j * 512, 512), 512)
                pxv[:, col] = dot(dqv[mine, :], wv[col, :], 1, 1).astype(BF16)

            tl.piece(0.2, key_grads)
            tl.loop(project_back, d // 512, 0.5)

        def weight_grads(n_t, g_t, u_t):
            g_t[...] = dot(n_t[...], dgv[...], 0, 0).astype(BF16)
            u_t[...] = dot(n_t[...], duv[...], 0, 0).astype(BF16)

        def weights(first, steps):
            tl.pipeline(weight_grads, steps, 2.4, [cols_spec(t, 256, first)], [rows_spec(256, f, first)] * 2, (n, dwg, dwu))

        def down_grad(do_t, out_t):
            out_t[...] = dot(hidv[...], do_t[...], 0, 0).astype(BF16)

        attention_half(1, 0.37)
        weights(0, 8)
        attention_half(0, 0.37)
        keep_o.start()
        keep_dqkv.start()
        weights(8, d // 256 - 8)
        tl.pipeline(down_grad, d // 512, 2.35, [cols_spec(t, 512)], [cols_spec(f, 512)], (d_out, dwd))
        tl.drain()

    pl.run_scoped(rest, pltpu.VMEM((d, c), BF16))
    keep_o.wait()
    keep_dqkv.wait()


def layer(part, h, d_out, stats, gains, n, hid_up, dg_up, du_up, wg, wu, wd, x, wqkv, wo, hd, tp):
    t, d = h.shape
    f = wg.shape[1]
    c = wqkv.shape[1]
    hw = wo.shape[0]
    rows = t // 2 // tp
    vm = lambda a, b, dt=BF16: pltpu.VMEM((a, b), dt)
    return pl.pallas_call(
        functools.partial(layer_body, rows=rows, hd=hd),
        in_specs=[ANY, ANY, ANY, IN_VMEM, IN_VMEM] + [ANY] * 10,
        out_specs=[ANY] * 8,
        out_shape=[shape_of((t, d)), shape_of((t, d)), shape_of((d, f)), shape_of((d, f)), shape_of((t, d)),
                   shape_of((f, d)), shape_of((t, hw)), shape_of((t, c))],
        scratch_shapes=[vm(t, f), vm(t, f), vm(t, f), vm(t, c), vm(t, c), vm(t, hw), vm(t // 2, hw),
                        vm(t // 2, d), vm(t // 2, d), vm(hw, d), vm(hd, t, F32), vm(hd, t, F32),
                        pltpu.SemaphoreType.DMA((10,)), pltpu.SemaphoreType.DMA((32,)),
                        pltpu.SemaphoreType.DMA((4 * COPIES,)), pltpu.SemaphoreType.DMA((4 * COPIES,))]
        + exchange_scratch(rows, d) * 2,
        compiler_params=pltpu.CompilerParams(vmem_limit_bytes=67043328, collective_id=1, has_side_effects=True),
        name="layer",
    )(part, h, d_out, stats, gains, n, hid_up, dg_up, du_up, wg, wu, wd, x, wqkv, wo)


def last_body(nx_ref, dqkv_ref, dm_ref, o_ref, dwg_in, dwu_in, dwd_in, dx_in,
              dwqkv_ref, dwo_ref, dwg_ref, dwu_ref, dwd_ref, dx_ref):
    dwg_ref[...] = dwg_in[...]
    dwu_ref[...] = dwu_in[...]
    dx_ref[...] = dx_in[...]
    dwd_ref[...] = dwd_in[...]
    dwqkv_ref[...] = dot(nx_ref[...], dqkv_ref[...], 0, 0).astype(BF16)
    dwo_ref[...] = dot(o_ref[...], dm_ref[...], 0, 0).astype(BF16)


def last(nx, dqkv, dmid, o, dwg, dwu, dwd, dx, block=512):
    t, d = nx.shape
    f, c, hw = dwg.shape[1], dqkv.shape[1], o.shape[1]
    steps = d // block
    moved = [rows_spec(block, f), rows_spec(block, f), rows_spec(f // steps, d), rows_spec(t // steps, d)]
    return pl.pallas_call(
        last_body,
        grid=(steps,),
        in_specs=[cols_spec(t, block), resident((t, c)), cols_spec(t, block),
                  resident((t, hw))] + moved,
        out_specs=[rows_spec(block, c), cols_spec(hw, block)] + moved,
        out_shape=[shape_of((d, c)), shape_of((hw, d)), shape_of((d, f)), shape_of((d, f)), shape_of((f, d)), shape_of((t, d))],
        compiler_params=params(),
        name="last",
    )(nx, dqkv, dmid, o, dwg, dwu, dwd, dx)


def solution(mesh):
    tp = mesh.shape["tp"]

    def device_step(x_in, h_mid, mean_x, rstd_x, mean_h, rstd_h, gain_x, gain_h, w_qkv, w_out, w_gate, w_up, w_down, d_out):
        heads, hd, d = w_out.shape
        stats = jnp.stack([mean_h, rstd_h, mean_x, rstd_x], axis=1)
        gains = jnp.stack([gain_h, gain_x]).astype(F32)
        hid_up, dg_up, du_up, norm_h = mlp_grads(h_mid, stats, gains, d_out, w_gate, w_up, w_down)
        part = mlp_part(dg_up, du_up, w_gate, w_up)
        d_mid, d_x, d_w_gate, d_w_up, norm_x, d_w_down, o, d_qkv = layer(
            part, h_mid, d_out, stats, gains, norm_h, hid_up, dg_up, du_up, w_gate, w_up, w_down, x_in, w_qkv,
            w_out.reshape(heads * hd, d), hd, tp)
        d_w_qkv, d_w_out, d_w_gate, d_w_up, d_w_down, d_x = last(norm_x, d_qkv, d_mid, o, d_w_gate, d_w_up, d_w_down, d_x)
        return d_x, d_w_qkv, d_w_out.reshape(w_out.shape), d_w_gate, d_w_up, d_w_down

    row_spec = P('dp', None)
    stat_spec = P('dp')
    col_spec = P(None, 'tp')
    in_specs = (row_spec, row_spec, stat_spec, stat_spec, stat_spec, stat_spec, P(None), P(None), col_spec, P('tp', None, None), col_spec, col_spec, P('tp', None), row_spec)
    out_specs = (row_spec, P('dp', 'tp'), P(('dp', 'tp'), None, None), P('dp', 'tp'), P('dp', 'tp'), P(('dp', 'tp'), None))
    return jax.shard_map(device_step, mesh=mesh, in_specs=in_specs, out_specs=out_specs, check_vma=False)
```
